32 devices in a mesh: parts: 2 (over y), sec: 16 (over z, x, core).
Axes of the slice: x: 2, y: 2, z: 4, core: 2. Of those that a mesh axis runs over, the one named last changes fastest.
Arguments:
- carry: bfloat16 [32, 96, 1152], P(('parts', 'sec')), parts along dimension 0, may hold values from -0.625 to 0.625
- site: bfloat16 [32, 96, 1536], P(('parts', 'sec')), parts along dimension 0, may hold values from -6 to 6
- mpo: bfloat16 [24, 16, 16, 12], P('parts'), parts along dimension 0, may hold values from -1.25 to 1.25
- omega: bfloat16 [1152, 128], replicated, may hold values from -0.1875 to 0.1875
- sector_sizes: int32 [32], P('parts'), parts along dimension 0, may hold values from 1 to 96, 768 in all
Outputs:
- left_factor: bfloat16 [32, 16, 96, 128], P(('parts', 'sec')), parts along dimension 0
- next_carry: bfloat16 [32, 128, 1152], P(('parts', 'sec')), parts along dimension 0
The draws below stay inside these ranges and needn't reach their ends.
There are 2 independent parts, one for each index of `parts`. The reference program is written for one: setup_inputs(seed, part) draws one part's arguments, and reference() takes and returns one part's arrays. A program takes and returns all parts, laid end to end along the dimension named above; an argument that names none is the same for every part. Nothing has to cross between parts.
Inputs may be any that keep to these rules, and one draw needn't show every extreme that they name: `sector_sizes`: they sum to 768 and the largest is exactly 96.
All inputs are finite; a program needn't handle non-finite values.
Results may differ from the reference program's by a relative error of at most 0.0095.
Values may be sent and summed in bfloat16 or wider, within the bound.
A program may use at most 64 MiB of HBM per device.

```python
import math
import jax
import jax.numpy as jnp
import numpy as np
from jax import lax

PHYS = 16
WM = 12
GRID_DN = 8
CAP = 96
SK = 128
NSEC = 16
CHI = 768


def steps_of(stream_key, extent, cuts, low, top_value):
    def one(axis_at, blocks):
        draws = jax.random.uniform(jax.random.fold_in(jax.random.fold_in(stream_key, 6), axis_at), (blocks,), jnp.float32, low / len(cuts), top_value / len(cuts))
        return jnp.repeat(jnp.exp(draws), extent[axis_at] // blocks).reshape((-1,) + (1,) * (len(extent) - axis_at - 1))

    level = one(*cuts[0])
    for cut in cuts[1:]:
        level = level * one(*cut)
    return level


def profile(amount, total, most, lean):
    weights = [(1 << 20) // math.isqrt(standing ** lean) + 1 for standing in range(2, amount + 1)]
    rest, given = total - most - (amount - 1), [1] * (amount - 1)
    while rest > 0:
        movable = [i for i in range(amount - 1) if given[i] < most]
        mass, remaining = sum([weights[i] for i in movable]), rest
        for i in movable:
            extra = min(most - given[i], max(1, remaining * weights[i] // mass), rest)
            given[i] = given[i] + extra
            rest = rest - extra
    return np.array([most] + given)


def ragged_sizes(key, count, total, most, slope):
    if count == 2:
        one = jax.random.randint(key, (), max(1, total - most), min(most, total - 1) + 1)
        return jnp.stack([one, total - one])
    lengths = jnp.asarray(profile(count, total, most, slope), jnp.int32)
    couples = (count - 1) // 2
    giver, receiver = lengths[1:1 + 2 * couples:2], lengths[2:2 + 2 * couples:2]
    room = jnp.minimum(giver - 1, most - receiver)
    moved = jax.random.randint(jax.random.fold_in(key, 1), (couples,), 0, 1 << 20) % (room + 1)
    lengths = lengths.at[1:1 + 2 * couples:2].set(giver - moved).at[2:2 + 2 * couples:2].set(receiver + moved)
    return lengths[jax.random.permutation(jax.random.fold_in(key, 2), count)]


def centred(key, shape, deviation, most, cuts=(), kind=jnp.bfloat16):
    values = deviation * jax.random.normal(key, shape, jnp.float32)
    if cuts:
        values = values * steps_of(key, shape, cuts, -0.22, 0.18)
    return jnp.clip(values, -most, most).astype(kind)


def setup_inputs(seed: int = 0, part: int = 0) -> dict:
    key_list = jax.random.split(jax.random.key(seed), 6)
    part_splits = jax.random.split(jax.random.fold_in(key_list[5], part), 6)
    carry = centred(part_splits[0], (NSEC, CAP, WM * CAP), CAP ** -0.5, 0.625, ((0, 16),))
    site = centred(part_splits[1], (NSEC, CAP, PHYS * CAP), 1.0, 6.0, ((0, 16),))
    mpo = centred(part_splits[2], (WM, PHYS, PHYS, WM), 24 ** -0.5, 1.25)
    omega = centred(key_list[3], (WM * CAP, SK), (WM * CAP) ** -0.5, 0.1875)
    sector_sizes = ragged_sizes(part_splits[4], NSEC, CHI, CAP, 2).astype(jnp.int32)
    return {"carry": carry, "site": site, "mpo": mpo, "omega": omega, "sector_sizes": sector_sizes}


def charge_tables():
    levels = np.array([-1, 0, 0, 1], np.int32)
    phys_up = np.repeat(levels, 4)
    phys_down = np.tile(levels, 4)
    bond_up = np.array([0, 0, 0, 0, 1, 1, -1, -1, 0, 0, 0, 0], np.int32)
    bond_down = np.array([0, 0, 0, 0, 0, 0, 0, 0, 1, 1, -1, -1], np.int32)
    return (phys_up, phys_down, bond_up, bond_down)

def conserving():
    phys_up, phys_down, bond_up, bond_down = charge_tables()
    left_up = bond_up[:, None, None, None] + phys_up[None, :, None, None]
    right_up = phys_up[None, None, :, None] + bond_up[None, None, None, :]
    left_down = bond_down[:, None, None, None] + phys_down[None, :, None, None]
    right_down = phys_down[None, None, :, None] + bond_down[None, None, None, :]
    return (left_up == right_up) & (left_down == right_down)

def inside(sector, shift_up, shift_down, count):
    upper = sector // GRID_DN + shift_up
    lower = sector % GRID_DN + shift_down
    return (upper >= 0) & (upper < count // GRID_DN) & (lower >= 0) & (lower < GRID_DN)

def orthonormal(sketch):
    gram = jnp.dot(sketch.T.astype(jnp.float32), sketch.astype(jnp.float32), precision=lax.Precision.HIGHEST, preferred_element_type=jnp.float32) / sketch.shape[0]
    ridge = 0.05 * jnp.trace(gram) / gram.shape[0] + 1e-06
    lower = jnp.linalg.cholesky(gram + ridge * jnp.eye(gram.shape[0], dtype=jnp.float32))
    solved = jax.scipy.linalg.solve_triangular(lower, sketch.T, lower=True)
    return solved.T.astype(jnp.bfloat16)

def reference(carry, site, mpo, omega, sector_sizes):
    phys_up, phys_down, bond_up, bond_down = charge_tables()
    phys_shift = jnp.asarray(phys_up * GRID_DN + phys_down)
    bond_shift = jnp.asarray(bond_up * GRID_DN + bond_down)
    sectors = jnp.arange(NSEC, dtype=jnp.int32)
    rows = jnp.arange(CAP, dtype=jnp.int32)
    live = rows[None, :] < sector_sizes[:, None]
    targets = sectors[:, None] + phys_shift[None, :]
    target_ok = inside(sectors[:, None], phys_up[None, :], phys_down[None, :], NSEC)
    target_sizes = sector_sizes[jnp.clip(targets, 0, NSEC - 1)]
    column_live = target_ok[:, :, None] & (rows[None, None, :] < target_sizes[:, :, None])
    site_four = site.reshape(NSEC, CAP, PHYS, CAP)
    site_masked = jnp.where(live[:, :, None, None] & column_live[:, None, :, :], site_four, jnp.zeros_like(site_four))
    source_ok = inside(sectors[:, None], -bond_up[None, :], -bond_down[None, :], NSEC)
    carry_four = carry.reshape(NSEC, CAP, WM, CAP)
    carry_masked = jnp.where(live[:, :, None, None] & source_ok[:, None, :, None], carry_four, jnp.zeros_like(carry_four))
    operator = jnp.where(jnp.asarray(conserving()), mpo.astype(jnp.float32), 0.0)

    def theta_of(sector):
        sources = jnp.clip(sector - bond_shift, 0, NSEC - 1)
        stacked = site_masked[sources].astype(jnp.float32)
        partial_sum = jnp.einsum('awj,wjsb->awsb', carry_masked[sector].astype(jnp.float32), stacked).astype(jnp.bfloat16)
        joined = jnp.einsum('awsb,wtsv->tavb', partial_sum.astype(jnp.float32), operator)
        keep = inside(sector, phys_up, phys_down, NSEC)
        joined = jnp.where(keep[:, None, None, None], joined, 0.0)
        return joined.astype(jnp.bfloat16).reshape(PHYS, CAP, WM * CAP)
    thetas = lax.map(theta_of, sectors)
    phys_index = jnp.arange(PHYS, dtype=jnp.int32)
    contract_rows = (((0,), (0,)), ((), ()))

    def solve_sector(sector):
        sources = jnp.clip(sector - phys_shift, 0, NSEC - 1)
        valid = inside(sector, -phys_up, -phys_down, NSEC)
        block = thetas[sources, phys_index]
        block = jnp.where(valid[:, None, None], block, jnp.zeros_like(block)).reshape(PHYS * CAP, WM * CAP)
        first_sketch = jnp.dot(block.astype(jnp.float32), omega.astype(jnp.float32), preferred_element_type=jnp.float32)
        basis = orthonormal(first_sketch)
        across = lax.dot_general(block.astype(jnp.float32), basis.astype(jnp.float32), contract_rows, preferred_element_type=jnp.float32).astype(jnp.bfloat16)
        second_sketch = jnp.dot(block.astype(jnp.float32), across.astype(jnp.float32), preferred_element_type=jnp.float32)
        left_basis = orthonormal(second_sketch)
        projected = lax.dot_general(left_basis.astype(jnp.float32), block.astype(jnp.float32), contract_rows, preferred_element_type=jnp.float32)
        return (left_basis.reshape(PHYS, CAP, SK), projected)
    left_factor, projected = lax.map(solve_sector, sectors)
    total = jnp.sum(projected * projected)
    next_carry = (projected * jnp.sqrt(NSEC / total)).astype(jnp.bfloat16)
    return (left_factor, next_carry)
```

```python
import functools
import jax
import jax.numpy as jnp
import numpy as np
from jax import lax
from jax.experimental import pallas as pl
from jax.experimental.pallas import tpu as pltpu
from jax.sharding import PartitionSpec as P

GRID_DN = 8


GROUPS = ((0, 4, 0, 0), (4, 6, 1, 0), (6, 8, -1, 0), (8, 10, 0, 1), (10, 12, 0, -1))
LEVELS = (-1, 0, 0, 1)
LEAF = 8
HIGH = lax.Precision.HIGHEST


def shifted(value, axis, steps):
    count = lax.axis_size(axis)
    initial, last = (max(0, -steps), min(count, count - steps))
    return lax.ppermute(value, axis, [(source, source + steps) for source in range(initial, last)])


def charge_tables():
    levels = np.array([-1, 0, 0, 1], np.int32)
    phys_up = np.repeat(levels, 4)
    phys_down = np.tile(levels, 4)
    bond_up = np.array([0, 0, 0, 0, 1, 1, -1, -1, 0, 0, 0, 0], np.int32)
    bond_down = np.array([0, 0, 0, 0, 0, 0, 0, 0, 1, 1, -1, -1], np.int32)
    return (phys_up, phys_down, bond_up, bond_down)


def conserving():
    phys_up, phys_down, bond_up, bond_down = charge_tables()
    left_up = bond_up[:, None, None, None] + phys_up[None, :, None, None]
    right_up = phys_up[None, None, :, None] + bond_up[None, None, None, :]
    left_down = bond_down[:, None, None, None] + phys_down[None, :, None, None]
    right_down = phys_down[None, None, :, None] + bond_down[None, None, None, :]
    return (left_up == right_up) & (left_down == right_down)


def inside(sector, shift_up, shift_down, count):
    upper = sector // GRID_DN + shift_up
    lower = sector % GRID_DN + shift_down
    return (upper >= 0) & (upper < count // GRID_DN) & (lower >= 0) & (lower < GRID_DN)


def inverse_factor(gram, work, leaf):
    size = gram.shape[0]
    eye = (
        lax.broadcasted_iota(jnp.int32, (size, size), 0)
        == lax.broadcasted_iota(jnp.int32, (size, size), 1)
    ).astype(jnp.float32)
    trace = jnp.sum(jnp.sum(gram * eye, axis=0, keepdims=True), axis=1, keepdims=True)
    ridge = 0.05 * trace / size + 1e-06
    work[:, :size] = gram + ridge * eye
    work[:, size:] = eye
    for first in range(0, size, LEAF):
        wide = []
        for i in range(LEAF):
            wide.append(work[first + i : first + i + 1, :])
        entry = [
            [
                jnp.broadcast_to(wide[i][:, first + k : first + k + 1], (1, 2 * size))
                for k in range(i + 1)
            ]
            for i in range(LEAF)
        ]
        for c in range(LEAF):
            inverse = lax.rsqrt(entry[c][c])
            wide[c] = wide[c] * inverse
            scaled = [entry[i][c] * inverse if i > c else None for i in range(LEAF)]
            for i in range(c + 1, LEAF):
                for k in range(c + 1, i + 1):
                    entry[i][k] = entry[i][k] - scaled[i] * scaled[k]
                wide[i] = wide[i] - scaled[i] * wide[c]
            leaf[c : c + 1, :] = wide[c]
        rows = leaf[...]
        if first + LEAF < size:
            rest = first + LEAF
            update = lax.dot_general(
                rows[:, :size],
                rows,
                (((0,), (0,)), ((), ())),
                precision=HIGH,
                preferred_element_type=jnp.float32,
            )
            work[rest:, :] = work[rest:, :] - update[rest:, :]
        work[first : first + LEAF, size:] = rows[:, size:]
    return work[:, size:]


def solve_kernel(
    count,
    theta,
    omega,
    left,
    carry_out,
    block,
    sketch,
    basis,
    across,
    projected,
    work,
    leaf,
    norms,
    norm_send,
    norm_recv,
    row_send,
    row_recv,
):
    me = lax.axis_index("sec")
    phys = theta.shape[0]
    capacity = theta.shape[1]
    rank = omega.shape[1]
    width = theta.shape[2]
    offsets = [(LEVELS[t // 4], LEVELS[t % 4]) for t in range(phys)]
    barrier = pltpu.get_barrier_semaphore()

    def greet(step, _):
        pl.semaphore_signal(barrier, inc=1, device_id={"sec": lax.rem(me + step, count)})
        return 0

    lax.fori_loop(1, count, greet, 0)
    pl.semaphore_wait(barrier, count - 1)

    def rows_of(t):
        return block.at[pl.ds(t * capacity, capacity)]

    def remote(t):
        up, down = offsets[t]
        return pltpu.make_async_remote_copy(
            src_ref=theta.at[t],
            dst_ref=rows_of(t),
            send_sem=row_send.at[t],
            recv_sem=row_recv.at[t],
            device_id={"sec": jnp.clip(me + up * GRID_DN + down, 0, count - 1)},
        )

    def local(t):
        return pltpu.make_async_copy(theta.at[t], rows_of(t), row_recv.at[t])

    order = sorted(range(phys), key=lambda t: (-abs(offsets[t][0]), -abs(offsets[t][1])))
    for t in order:
        up, down = offsets[t]
        if up == 0 and down == 0:
            local(t).start()
        else:

            @pl.when(inside(me, up, down, count))
            def _(t=t):
                remote(t).start()

    for t in reversed(order):
        up, down = offsets[t]
        rows = pl.ds(t * capacity, capacity)
        if up == 0 and down == 0:
            local(t).wait()
        else:
            arrives = inside(me, -up, -down, count)

            @pl.when(arrives)
            def _(t=t):
                remote(t).wait_recv()

            @pl.when(jnp.logical_not(arrives))
            def _(t=t, rows=rows):
                block[rows, :] = jnp.zeros((capacity, width), block.dtype)

        sketch[rows, :] = jnp.dot(
            block[rows, :], omega[...], preferred_element_type=jnp.float32
        )
    for t in order:
        up, down = offsets[t]
        if up != 0 or down != 0:

            @pl.when(inside(me, up, down, count))
            def _(t=t):
                remote(t).wait_send()

    def orthonormal(out):
        gram = lax.dot_general(
            sketch[...],
            sketch[...],
            (((0,), (0,)), ((), ())),
            precision=HIGH,
            preferred_element_type=jnp.float32,
        ) / (phys * capacity)
        inverse = inverse_factor(gram, work, leaf)
        out[...] = lax.dot_general(
            sketch[...],
            inverse,
            (((1,), (1,)), ((), ())),
            precision=HIGH,
            preferred_element_type=jnp.float32,
        ).astype(out.dtype)

    def project(factor, out):
        out[...] = lax.dot_general(
            factor[...],
            block[...],
            (((0,), (0,)), ((), ())),
            preferred_element_type=jnp.float32,
        ).astype(out.dtype)

    orthonormal(basis)
    project(basis, across)
    sketch[...] = lax.dot_general(
        block[...], across[...], (((1,), (1,)), ((), ())), preferred_element_type=jnp.float32
    )
    orthonormal(basis)
    left[...] = basis[...]
    project(basis, projected)
    squares = projected[...] * projected[...]
    partial = jnp.sum(squares.reshape(rank // 8, 8, width), axis=0)
    folded = partial[:, :128]
    for first in range(128, width, 128):
        folded = folded + partial[:, first : first + 128]
    norms[me] = folded

    def share(step):
        return pltpu.make_async_remote_copy(
            src_ref=norms.at[me],
            dst_ref=norms.at[me],
            send_sem=norm_send.at[step],
            recv_sem=norm_recv.at[step],
            device_id={"sec": lax.rem(me + step, count)},
        )

    def begin(step, _):
        share(step).start()
        return 0

    def finish(step, _):
        share(step).wait()
        return 0

    lax.fori_loop(1, count, begin, 0)
    lax.fori_loop(1, count, finish, 0)
    summed = jnp.sum(norms[...], axis=0)
    total = jnp.sum(jnp.sum(summed, axis=0, keepdims=True), axis=1, keepdims=True)
    carry_out[...] = (projected[...] * jnp.sqrt(count / total)).astype(carry_out.dtype)


def solve(theta, omega, count):
    phys, capacity, width = theta.shape
    rank = omega.shape[1]
    rows = phys * capacity
    vmem = pl.BlockSpec(memory_space=pltpu.VMEM)
    return pl.pallas_call(
        functools.partial(solve_kernel, count),
        out_shape=(
            jax.ShapeDtypeStruct((rows, rank), jnp.bfloat16),
            jax.ShapeDtypeStruct((rank, width), jnp.bfloat16),
        ),
        in_specs=[pl.BlockSpec(memory_space=pl.ANY), vmem],
        out_specs=(vmem, vmem),
        scratch_shapes=[
            pltpu.VMEM((rows, width), jnp.bfloat16),
            pltpu.VMEM((rows, rank), jnp.float32),
            pltpu.VMEM((rows, rank), jnp.bfloat16),
            pltpu.VMEM((rank, width), jnp.bfloat16),
            pltpu.VMEM((rank, width), jnp.float32),
            pltpu.VMEM((rank, 2 * rank), jnp.float32),
            pltpu.VMEM((LEAF, 2 * rank), jnp.float32),
            pltpu.VMEM((count, 8, 128), jnp.float32),
            pltpu.SemaphoreType.DMA((count,)),
            pltpu.SemaphoreType.DMA((count,)),
            pltpu.SemaphoreType.DMA((phys,)),
            pltpu.SemaphoreType.DMA((phys,)),
        ],
        compiler_params=pltpu.CompilerParams(
            collective_id=0, has_side_effects=True, vmem_limit_bytes=40 * 1024 * 1024
        ),
        name="solve",
    )(theta, omega)


def body(carry, site, mpo, omega, sector_sizes):
    count = lax.axis_size("sec")
    sector = lax.axis_index("sec")
    capacity = carry.shape[1]
    bond_width = mpo.shape[0]
    phys_width = mpo.shape[1]
    phys_up, phys_down, bond_up, bond_down = charge_tables()
    rows = jnp.arange(capacity, dtype=jnp.int32)
    own_live = rows < sector_sizes[sector]
    targets = sector + jnp.asarray(phys_up * GRID_DN + phys_down)
    target_ok = inside(sector, phys_up, phys_down, count)
    target_sizes = sector_sizes[jnp.clip(targets, 0, count - 1)]
    column_live = target_ok[:, None] & (rows[None, :] < target_sizes[:, None])
    site_four = site[0].reshape(capacity, phys_width, capacity)
    site_masked = jnp.where(
        own_live[:, None, None] & column_live[None, :, :], site_four, jnp.zeros_like(site_four)
    )
    site_masked = site_masked.reshape(capacity, phys_width * capacity)
    carry_three = jnp.where(own_live[:, None], carry[0], jnp.zeros_like(carry[0])).reshape(
        capacity, bond_width, capacity
    )
    pieces = []
    for first_bond, last_bond, shift_up, shift_down in GROUPS:
        offset = shift_up * GRID_DN + shift_down
        source = site_masked if offset == 0 else shifted(site_masked, "sec", offset)
        valid = inside(sector, -shift_up, -shift_down, count)
        carry_part = carry_three[:, first_bond:last_bond]
        carry_part = jnp.where(valid, carry_part, jnp.zeros_like(carry_part))
        group_width = last_bond - first_bond
        product = jnp.dot(
            carry_part.reshape(capacity * group_width, capacity),
            source,
            preferred_element_type=jnp.float32,
        )
        pieces.append(product.reshape(capacity, group_width, phys_width * capacity))
    partial_sum = (
        jnp.concatenate(pieces, 1)
        .astype(jnp.bfloat16)
        .reshape(capacity, bond_width, phys_width, capacity)
    )
    operator = jnp.where(jnp.asarray(conserving()), mpo, jnp.zeros_like(mpo))
    joined = jnp.einsum(
        "awsb,wtsv->tavb", partial_sum, operator, preferred_element_type=jnp.float32
    )
    joined = jnp.where(target_ok[:, None, None, None], joined, 0.0).astype(jnp.bfloat16)
    theta = joined.reshape(phys_width, capacity, bond_width * capacity)
    left, next_carry = solve(theta, omega, count)
    return (left.reshape(1, phys_width, capacity, omega.shape[1]), next_carry[None])


def solution(mesh):
    return jax.shard_map(
        body,
        mesh=mesh,
        in_specs=(
            P(("parts", "sec"), None, None),
            P(("parts", "sec"), None, None),
            P("parts", None, None, None),
            P(),
            P("parts"),
        ),
        out_specs=(P(("parts", "sec"), None, None, None), P(("parts", "sec"), None, None)),
        check_vma=False,
    )
```

```python
import functools
import jax
import jax.numpy as jnp
import numpy as np
from jax import lax
from jax.experimental import pallas as pl
from jax.experimental.pallas import tpu as pltpu
from jax.sharding import PartitionSpec as P

GRID_DN = 8


GROUPS = ((0, 4, 0, 0), (4, 6, 1, 0), (6, 8, -1, 0), (8, 10, 0, 1), (10, 12, 0, -1))
LEVELS = (-1, 0, 0, 1)
LEAF = 8
HIGH = lax.Precision.HIGHEST


def shifted(value, axis, steps):
    count = lax.axis_size(axis)
    initial, last = (max(0, -steps), min(count, count - steps))
    return lax.ppermute(value, axis, [(source, source + steps) for source in range(initial, last)])


def charge_tables():
    levels = np.array([-1, 0, 0, 1], np.int32)
    phys_up = np.repeat(levels, 4)
    phys_down = np.tile(levels, 4)
    bond_up = np.array([0, 0, 0, 0, 1, 1, -1, -1, 0, 0, 0, 0], np.int32)
    bond_down = np.array([0, 0, 0, 0, 0, 0, 0, 0, 1, 1, -1, -1], np.int32)
    return (phys_up, phys_down, bond_up, bond_down)


def conserving():
    phys_up, phys_down, bond_up, bond_down = charge_tables()
    left_up = bond_up[:, None, None, None] + phys_up[None, :, None, None]
    right_up = phys_up[None, None, :, None] + bond_up[None, None, None, :]
    left_down = bond_down[:, None, None, None] + phys_down[None, :, None, None]
    right_down = phys_down[None, None, :, None] + bond_down[None, None, None, :]
    return (left_up == right_up) & (left_down == right_down)


def inside(sector, shift_up, shift_down, count):
    upper = sector // GRID_DN + shift_up
    lower = sector % GRID_DN + shift_down
    return (upper >= 0) & (upper < count // GRID_DN) & (lower >= 0) & (lower < GRID_DN)


def inverse_factor(gram, work, leaf):
    size = gram.shape[0]
    eye = (
        lax.broadcasted_iota(jnp.int32, (size, size), 0)
        == lax.broadcasted_iota(jnp.int32, (size, size), 1)
    ).astype(jnp.float32)
    trace = jnp.sum(jnp.sum(gram * eye, axis=0, keepdims=True), axis=1, keepdims=True)
    ridge = 0.05 * trace / size + 1e-06
    work[:, :size] = gram + ridge * eye
    work[:, size:] = eye
    for first in range(0, size, LEAF):
        wide = []
        for i in range(LEAF):
            wide.append(work[first + i : first + i + 1, :])
        entry = [
            [
                jnp.broadcast_to(wide[i][:, first + k : first + k + 1], (1, 2 * size))
                for k in range(i + 1)
            ]
            for i in range(LEAF)
        ]
        for c in range(LEAF):
            inverse = lax.rsqrt(entry[c][c])
            wide[c] = wide[c] * inverse
            scaled = [entry[i][c] * inverse if i > c else None for i in range(LEAF)]
            for i in range(c + 1, LEAF):
                for k in range(c + 1, i + 1):
                    entry[i][k] = entry[i][k] - scaled[i] * scaled[k]
                wide[i] = wide[i] - scaled[i] * wide[c]
            leaf[c : c + 1, :] = wide[c]
        rows = leaf[...]
        if first + LEAF < size:
            rest = first + LEAF
            update = lax.dot_general(
                rows[:, :size],
                rows,
                (((0,), (0,)), ((), ())),
                precision=HIGH,
                preferred_element_type=jnp.float32,
            )
            work[rest:, :] = work[rest:, :] - update[rest:, :]
        work[first : first + LEAF, size:] = rows[:, size:]
    return work[:, size:]


def solve_kernel(
    count,
    theta,
    omega,
    left,
    carry_out,
    block,
    sketch,
    basis,
    across,
    projected,
    work,
    leaf,
    norms,
    norm_send,
    norm_recv,
    row_send,
    row_recv,
):
    me = lax.axis_index("sec")
    phys = theta.shape[0]
    capacity = theta.shape[1]
    rank = omega.shape[1]
    width = theta.shape[2]
    offsets = [(LEVELS[t // 4], LEVELS[t % 4]) for t in range(phys)]
    barrier = pltpu.get_barrier_semaphore()

    def greet(step, _):
        pl.semaphore_signal(barrier, inc=1, device_id={"sec": lax.rem(me + step, count)})
        return 0

    lax.fori_loop(1, count, greet, 0)
    pl.semaphore_wait(barrier, count - 1)

    def rows_of(t):
        return block.at[pl.ds(t * capacity, capacity)]

    def remote(t):
        up, down = offsets[t]
        return pltpu.make_async_remote_copy(
            src_ref=theta.at[t],
            dst_ref=rows_of(t),
            send_sem=row_send.at[t],
            recv_sem=row_recv.at[t],
            device_id={"sec": jnp.clip(me + up * GRID_DN + down, 0, count - 1)},
        )

    def local(t):
        return pltpu.make_async_copy(theta.at[t], rows_of(t), row_recv.at[t])

    order = sorted(range(phys), key=lambda t: (-abs(offsets[t][0]), -abs(offsets[t][1])))
    for t in order:
        up, down = offsets[t]
        if up == 0 and down == 0:
            local(t).start()
        else:

            @pl.when(inside(me, up, down, count))
            def _(t=t):
                remote(t).start()

    for t in reversed(order):
        up, down = offsets[t]
        rows = pl.ds(t * capacity, capacity)
        if up == 0 and down == 0:
            local(t).wait()
        else:
            arrives = inside(me, -up, -down, count)

            @pl.when(arrives)
            def _(t=t):
                remote(t).wait_recv()

            @pl.when(jnp.logical_not(arrives))
            def _(t=t, rows=rows):
                block[rows, :] = jnp.zeros((capacity, width), block.dtype)

        sketch[rows, :] = jnp.dot(
            block[rows, :], omega[...], preferred_element_type=jnp.float32
        )
    for t in order:
        up, down = offsets[t]
        if up != 0 or down != 0:

            @pl.when(inside(me, up, down, count))
            def _(t=t):
                remote(t).wait_send()

    def orthonormal(out):
        gram = lax.dot_general(
            sketch[...],
            sketch[...],
            (((0,), (0,)), ((), ())),
            precision=HIGH,
            preferred_element_type=jnp.float32,
        ) / (phys * capacity)
        inverse = inverse_factor(gram, work, leaf)
        out[...] = lax.dot_general(
            sketch[...],
            inverse,
            (((1,), (1,)), ((), ())),
            precision=HIGH,
            preferred_element_type=jnp.float32,
        ).astype(out.dtype)

    def project(factor, out):
        out[...] = lax.dot_general(
            factor[...],
            block[...],
            (((0,), (0,)), ((), ())),
            preferred_element_type=jnp.float32,
        ).astype(out.dtype)

    orthonormal(basis)
    project(basis, across)
    sketch[...] = lax.dot_general(
        block[...], across[...], (((1,), (1,)), ((), ())), preferred_element_type=jnp.float32
    )
    orthonormal(basis)
    left[...] = basis[...]
    project(basis, projected)
    squares = projected[...] * projected[...]
    partial = jnp.sum(squares.reshape(rank // 8, 8, width), axis=0)
    folded = partial[:, :128]
    for first in range(128, width, 128):
        folded = folded + partial[:, first : first + 128]
    norms[me] = folded

    def share(step):
        return pltpu.make_async_remote_copy(
            src_ref=norms.at[me],
            dst_ref=norms.at[me],
            send_sem=norm_send.at[step],
            recv_sem=norm_recv.at[step],
            device_id={"sec": lax.rem(me + step, count)},
        )

    def begin(step, _):
        share(step).start()
        return 0

    def finish(step, _):
        share(step).wait()
        return 0

    lax.fori_loop(1, count, begin, 0)
    lax.fori_loop(1, count, finish, 0)
    summed = jnp.sum(norms[...], axis=0)
    total = jnp.sum(jnp.sum(summed, axis=0, keepdims=True), axis=1, keepdims=True)
    carry_out[...] = (projected[...] * jnp.sqrt(count / total)).astype(carry_out.dtype)


def solve(theta, omega, count):
    phys, capacity, width = theta.shape
    rank = omega.shape[1]
    rows = phys * capacity
    vmem = pl.BlockSpec(memory_space=pltpu.VMEM)
    return pl.pallas_call(
        functools.partial(solve_kernel, count),
        out_shape=(
            jax.ShapeDtypeStruct((rows, rank), jnp.bfloat16),
            jax.ShapeDtypeStruct((rank, width), jnp.bfloat16),
        ),
        in_specs=[pl.BlockSpec(memory_space=pl.ANY), vmem],
        out_specs=(vmem, vmem),
        scratch_shapes=[
            pltpu.VMEM((rows, width), jnp.bfloat16),
            pltpu.VMEM((rows, rank), jnp.float32),
            pltpu.VMEM((rows, rank), jnp.bfloat16),
            pltpu.VMEM((rank, width), jnp.bfloat16),
            pltpu.VMEM((rank, width), jnp.float32),
            pltpu.VMEM((rank, 2 * rank), jnp.float32),
            pltpu.VMEM((LEAF, 2 * rank), jnp.float32),
            pltpu.VMEM((count, 8, 128), jnp.float32),
            pltpu.SemaphoreType.DMA((count,)),
            pltpu.SemaphoreType.DMA((count,)),
            pltpu.SemaphoreType.DMA((phys,)),
            pltpu.SemaphoreType.DMA((phys,)),
        ],
        compiler_params=pltpu.CompilerParams(
            collective_id=0, has_side_effects=True, vmem_limit_bytes=40 * 1024 * 1024
        ),
        name="solve",
    )(theta, omega)


def theta_kernel(carry, matrix, live, own, *rest):
    sites = (own,) + rest[:4]
    theta, parts, rows = rest[4:]
    width, capacity = carry.shape[0], carry.shape[1]
    phys = theta.shape[0]
    pairs = width * phys
    pad = jnp.zeros((capacity, 128 - capacity % 128), own.dtype)
    for s in range(phys):
        for (first, last, _, _), source in zip(GROUPS, sites):
            piece = jnp.concatenate([source[:, s * capacity : (s + 1) * capacity], pad], 1)
            product = jnp.dot(
                carry[first:last].reshape((last - first) * capacity, capacity),
                piece,
                preferred_element_type=jnp.float32,
            )
            for w in range(first, last):
                at = (w - first) * capacity
                parts[pl.ds(w * phys + s, capacity, stride=PITCH), :] = product[at : at + capacity]

    def apply(step, _):
        for inner in range(0, UNROLL, 2):
            a = step * UNROLL + inner
            pair = [
                parts[pl.ds(pl.multiple_of((a + k) * PITCH, 8), pairs), :].astype(jnp.bfloat16)
                for k in range(2)
            ]
            out = jnp.dot(
                matrix[...], jnp.concatenate(pair, 1), preferred_element_type=jnp.float32
            )
            for k in range(2):
                for v in range(width):
                    rows[pl.ds(v * phys * capacity + a + k, phys, stride=capacity), :] = out[
                        v * phys : (v + 1) * phys, k * 128 : (k + 1) * 128
                    ]
        return 0

    lax.fori_loop(0, capacity // UNROLL, apply, 0)

    def finish(t, _):
        pieces = [
            rows[pl.ds(pl.multiple_of((v * phys + t) * capacity, 8), capacity), :][:, :capacity]
            for v in range(width)
        ]
        joined = jnp.concatenate(pieces, 1)
        theta[t] = jnp.where(live[t] > 0.5, joined, 0.0).astype(theta.dtype)
        return 0

    lax.fori_loop(0, phys, finish, 0)


PITCH = 200
UNROLL = 8


def make_theta(carry, matrix, live, sites):
    width, capacity = carry.shape[0], carry.shape[1]
    phys = live.shape[0]
    vmem = pl.BlockSpec(memory_space=pltpu.VMEM)
    return pl.pallas_call(
        theta_kernel,
        out_shape=jax.ShapeDtypeStruct((phys, capacity, width * capacity), jnp.bfloat16),
        in_specs=[vmem] * (3 + len(sites)),
        out_specs=vmem,
        scratch_shapes=[
            pltpu.VMEM((PITCH * capacity, 128), jnp.float32),
            pltpu.VMEM((width * phys * capacity, 128), jnp.float32),
        ],
        compiler_params=pltpu.CompilerParams(vmem_limit_bytes=48 * 1024 * 1024),
        name="theta",
    )(carry, matrix, live, *sites)


def body(carry, site, mpo, omega, sector_sizes):
    count = lax.axis_size("sec")
    sector = lax.axis_index("sec")
    capacity = carry.shape[1]
    bond_width = mpo.shape[0]
    phys_width = mpo.shape[1]
    raw = site[0]
    sites = [raw] + [shifted(raw, "sec", up * GRID_DN + down) for _, _, up, down in GROUPS[1:]]
    phys_up, phys_down, bond_up, bond_down = charge_tables()
    rows = jnp.arange(capacity, dtype=jnp.int32)

    def sizes_at(up, down):
        at = jnp.clip(sector + jnp.asarray(up * GRID_DN + down), 0, count - 1)
        hit = at[..., None] == jnp.arange(count, dtype=jnp.int32)
        found = jnp.sum(jnp.where(hit, sector_sizes, 0), -1)
        return jnp.where(inside(sector, up, down, count), found, 0)

    own_size = sizes_at(np.zeros((1,), np.int32), np.zeros((1,), np.int32))
    source_sizes = sizes_at(-bond_up, -bond_down)
    carry_live = (rows[None, :, None] < own_size) & (
        rows[None, None, :] < source_sizes[:, None, None]
    )
    carry_three = carry[0].reshape(capacity, bond_width, capacity).transpose(1, 0, 2)
    carry_three = jnp.where(carry_live, carry_three, jnp.zeros_like(carry_three))
    column_sizes = sizes_at(
        phys_up[:, None] - bond_up[None, :], phys_down[:, None] - bond_down[None, :]
    )
    target_ok = inside(sector, phys_up, phys_down, count)
    live = (rows[None, None, :] < column_sizes[:, :, None]) & target_ok[:, None, None]
    live = live.astype(jnp.float32).reshape(phys_width, 1, bond_width * capacity)
    operator = jnp.where(jnp.asarray(conserving()), mpo, jnp.zeros_like(mpo))
    pairs = phys_width * bond_width
    matrix = operator.transpose(3, 1, 0, 2).reshape(pairs, pairs)
    theta = make_theta(carry_three, matrix, live, sites)
    left, next_carry = solve(theta, omega, count)
    return (left.reshape(1, phys_width, capacity, omega.shape[1]), next_carry[None])


def solution(mesh):
    return jax.shard_map(
        body,
        mesh=mesh,
        in_specs=(
            P(("parts", "sec"), None, None),
            P(("parts", "sec"), None, None),
            P("parts", None, None, None),
            P(),
            P("parts"),
        ),
        out_specs=(P(("parts", "sec"), None, None, None), P(("parts", "sec"), None, None)),
        check_vma=False,
    )
```

```python
import functools
import jax
import jax.numpy as jnp
import numpy as np
from jax import lax
from jax.experimental import pallas as pl
from jax.experimental.pallas import tpu as pltpu
from jax.sharding import PartitionSpec as P

GRID_DN = 8


GROUPS = ((0, 4, 0, 0), (4, 6, 1, 0), (6, 8, -1, 0), (8, 10, 0, 1), (10, 12, 0, -1))
LEVELS = (-1, 0, 0, 1)
LEAF = 8
HIGH = lax.Precision.HIGHEST


def shifted(value, axis, steps):
    count = lax.axis_size(axis)
    initial, last = (max(0, -steps), min(count, count - steps))
    return lax.ppermute(value, axis, [(source, source + steps) for source in range(initial, last)])


def charge_tables():
    levels = np.array([-1, 0, 0, 1], np.int32)
    phys_up = np.repeat(levels, 4)
    phys_down = np.tile(levels, 4)
    bond_up = np.array([0, 0, 0, 0, 1, 1, -1, -1, 0, 0, 0, 0], np.int32)
    bond_down = np.array([0, 0, 0, 0, 0, 0, 0, 0, 1, 1, -1, -1], np.int32)
    return (phys_up, phys_down, bond_up, bond_down)


def conserving():
    phys_up, phys_down, bond_up, bond_down = charge_tables()
    left_up = bond_up[:, None, None, None] + phys_up[None, :, None, None]
    right_up = phys_up[None, None, :, None] + bond_up[None, None, None, :]
    left_down = bond_down[:, None, None, None] + phys_down[None, :, None, None]
    right_down = phys_down[None, None, :, None] + bond_down[None, None, None, :]
    return (left_up == right_up) & (left_down == right_down)


def inside(sector, shift_up, shift_down, count):
    upper = sector // GRID_DN + shift_up
    lower = sector % GRID_DN + shift_down
    return (upper >= 0) & (upper < count // GRID_DN) & (lower >= 0) & (lower < GRID_DN)


def inverse_factor(gram, work, leaf):
    size = gram.shape[0]
    eye = (
        lax.broadcasted_iota(jnp.int32, (size, size), 0)
        == lax.broadcasted_iota(jnp.int32, (size, size), 1)
    ).astype(jnp.float32)
    trace = jnp.sum(jnp.sum(gram * eye, axis=0, keepdims=True), axis=1, keepdims=True)
    ridge = 0.05 * trace / size + 1e-06
    work[:, :size] = gram + ridge * eye
    work[:, size:] = eye
    for first in range(0, size, LEAF):
        wide = []
        for i in range(LEAF):
            wide.append(work[first + i : first + i + 1, :])
        entry = [
            [
                jnp.broadcast_to(wide[i][:, first + k : first + k + 1], (1, 2 * size))
                for k in range(i + 1)
            ]
            for i in range(LEAF)
        ]
        for c in range(LEAF):
            inverse = lax.rsqrt(entry[c][c])
            wide[c] = wide[c] * inverse
            scaled = [entry[i][c] * inverse if i > c else None for i in range(LEAF)]
            for i in range(c + 1, LEAF):
                for k in range(c + 1, i + 1):
                    entry[i][k] = entry[i][k] - scaled[i] * scaled[k]
                wide[i] = wide[i] - scaled[i] * wide[c]
            leaf[c : c + 1, :] = wide[c]
        rows = leaf[...]
        if first + LEAF < size:
            rest = first + LEAF
            update = lax.dot_general(
                rows[:, :size],
                rows,
                (((0,), (0,)), ((), ())),
                precision=HIGH,
                preferred_element_type=jnp.float32,
            )
            work[rest:, :] = work[rest:, :] - update[rest:, :]
        work[first : first + LEAF, size:] = rows[:, size:]
    return work[:, size:]


def solve_kernel(count, paired, n_theta, *refs):
    thetas, omega = refs[:n_theta], refs[n_theta]
    (
        left,
        carry_out,
        block,
        sketch,
        basis,
        across,
        projected,
        work,
        leaf,
        norms,
        norm_send,
        norm_recv,
        row_send,
        row_recv,
    ) = refs[n_theta + 1 :]
    me = lax.axis_index("sec")
    capacity = thetas[0].shape[1]
    phys = block.shape[0] // capacity
    rank = omega.shape[1]
    width = block.shape[1]
    if paired:
        inner, swapped = thetas
        crossing = swapped.shape[0]
        entry_row = (me // GRID_DN) * (phys - crossing)
        items = [(swapped.at[k], entry_row + k, 0, LEVELS[k]) for k in range(crossing)] + [
            (inner.at[k], crossing + k, 0, LEVELS[(crossing + k) % 4])
            for k in range(inner.shape[0])
        ]
    else:
        items = [(thetas[0].at[t], t, LEVELS[t // 4], LEVELS[t % 4]) for t in range(phys)]
    barrier = pltpu.get_barrier_semaphore()

    def greet(step, _):
        pl.semaphore_signal(barrier, inc=1, device_id={"sec": lax.rem(me + step, count)})
        return 0

    lax.fori_loop(1, count, greet, 0)
    pl.semaphore_wait(barrier, count - 1)

    def rows_of(n):
        start = items[n][1] * capacity
        return pl.ds(start if isinstance(start, int) else pl.multiple_of(start, 16), capacity)

    def remote(n):
        source, _, up, down = items[n]
        return pltpu.make_async_remote_copy(
            src_ref=source,
            dst_ref=block.at[rows_of(n)],
            send_sem=row_send.at[n],
            recv_sem=row_recv.at[n],
            device_id={"sec": jnp.clip(me + up * GRID_DN + down, 0, count - 1)},
        )

    def local(n):
        return pltpu.make_async_copy(items[n][0], block.at[rows_of(n)], row_recv.at[n])

    order = sorted(range(len(items)), key=lambda n: (-abs(items[n][2]), -abs(items[n][3])))
    for n in order:
        _, _, up, down = items[n]
        if up == 0 and down == 0:
            local(n).start()
        else:

            @pl.when(inside(me, up, down, count))
            def _(n=n):
                remote(n).start()

    if paired:
        empty = pl.ds(
            pl.multiple_of((phys - crossing - entry_row) * capacity, 16), crossing * capacity
        )
        block[empty, :] = jnp.zeros((crossing * capacity, width), block.dtype)
        sketch[empty, :] = jnp.zeros((crossing * capacity, rank), sketch.dtype)
    for n in reversed(order):
        _, _, up, down = items[n]
        rows = rows_of(n)
        if up == 0 and down == 0:
            local(n).wait()
        else:
            arrives = inside(me, -up, -down, count)

            @pl.when(arrives)
            def _(n=n):
                remote(n).wait_recv()

            @pl.when(jnp.logical_not(arrives))
            def _(rows=rows):
                block[rows, :] = jnp.zeros((capacity, width), block.dtype)

        sketch[rows, :] = jnp.dot(
            block[rows, :], omega[...], preferred_element_type=jnp.float32
        )
    for n in order:
        _, _, up, down = items[n]
        if up != 0 or down != 0:

            @pl.when(inside(me, up, down, count))
            def _(n=n):
                remote(n).wait_send()

    def orthonormal(out):
        gram = lax.dot_general(
            sketch[...],
            sketch[...],
            (((0,), (0,)), ((), ())),
            precision=HIGH,
            preferred_element_type=jnp.float32,
        ) / (phys * capacity)
        inverse = inverse_factor(gram, work, leaf)
        out[...] = lax.dot_general(
            sketch[...],
            inverse,
            (((1,), (1,)), ((), ())),
            precision=HIGH,
            preferred_element_type=jnp.float32,
        ).astype(out.dtype)

    def project(factor, out):
        out[...] = lax.dot_general(
            factor[...],
            block[...],
            (((0,), (0,)), ((), ())),
            preferred_element_type=jnp.float32,
        ).astype(out.dtype)

    orthonormal(basis)
    project(basis, across)
    sketch[...] = lax.dot_general(
        block[...], across[...], (((1,), (1,)), ((), ())), preferred_element_type=jnp.float32
    )
    orthonormal(basis)
    left[...] = basis[...]
    project(basis, projected)
    squares = projected[...] * projected[...]
    partial = jnp.sum(squares.reshape(rank // 8, 8, width), axis=0)
    folded = partial[:, :128]
    for first in range(128, width, 128):
        folded = folded + partial[:, first : first + 128]
    norms[me] = folded

    def share(step):
        return pltpu.make_async_remote_copy(
            src_ref=norms.at[me],
            dst_ref=norms.at[me],
            send_sem=norm_send.at[step],
            recv_sem=norm_recv.at[step],
            device_id={"sec": lax.rem(me + step, count)},
        )

    def begin(step, _):
        share(step).start()
        return 0

    def finish(step, _):
        share(step).wait()
        return 0

    lax.fori_loop(1, count, begin, 0)
    lax.fori_loop(1, count, finish, 0)
    summed = jnp.sum(norms[...], axis=0)
    total = jnp.sum(jnp.sum(summed, axis=0, keepdims=True), axis=1, keepdims=True)
    carry_out[...] = (projected[...] * jnp.sqrt(count / total)).astype(carry_out.dtype)


def solve(thetas, omega, count, phys):
    _, capacity, width = thetas[0].shape
    rank = omega.shape[1]
    rows = phys * capacity
    vmem = pl.BlockSpec(memory_space=pltpu.VMEM)
    return pl.pallas_call(
        functools.partial(solve_kernel, count, len(thetas) > 1, len(thetas)),
        out_shape=(
            jax.ShapeDtypeStruct((rows, rank), jnp.bfloat16),
            jax.ShapeDtypeStruct((rank, width), jnp.bfloat16),
        ),
        in_specs=[pl.BlockSpec(memory_space=pl.ANY)] * len(thetas) + [vmem],
        out_specs=(vmem, vmem),
        scratch_shapes=[
            pltpu.VMEM((rows, width), jnp.bfloat16),
            pltpu.VMEM((rows, rank), jnp.float32),
            pltpu.VMEM((rows, rank), jnp.bfloat16),
            pltpu.VMEM((rank, width), jnp.bfloat16),
            pltpu.VMEM((rank, width), jnp.float32),
            pltpu.VMEM((rank, 2 * rank), jnp.float32),
            pltpu.VMEM((LEAF, 2 * rank), jnp.float32),
            pltpu.VMEM((count, 8, 128), jnp.float32),
            pltpu.SemaphoreType.DMA((count,)),
            pltpu.SemaphoreType.DMA((count,)),
            pltpu.SemaphoreType.DMA((phys,)),
            pltpu.SemaphoreType.DMA((phys,)),
        ],
        compiler_params=pltpu.CompilerParams(
            collective_id=0, has_side_effects=True, vmem_limit_bytes=40 * 1024 * 1024
        ),
        name="solve",
    )(*thetas, omega)


def theta_kernel(carry, matrix, live, own, *rest):
    sites = (own,) + rest[:4]
    theta, parts, rows = rest[4:]
    width, capacity = carry.shape[0], carry.shape[1]
    phys = own.shape[1] // capacity
    pairs = width * phys
    outs = matrix.shape[0] // width
    pad = jnp.zeros((capacity, 128 - capacity % 128), own.dtype)
    for s in range(phys):
        for (first, last, _, _), source in zip(GROUPS, sites):
            piece = jnp.concatenate([source[:, s * capacity : (s + 1) * capacity], pad], 1)
            product = jnp.dot(
                carry[first:last].reshape((last - first) * capacity, capacity),
                piece,
                preferred_element_type=jnp.float32,
            )
            for w in range(first, last):
                at = (w - first) * capacity
                parts[pl.ds(w * phys + s, capacity, stride=PITCH), :] = product[at : at + capacity]

    def apply(step, _):
        for inner in range(0, UNROLL, 2):
            a = step * UNROLL + inner
            pair = [
                parts[pl.ds(pl.multiple_of((a + k) * PITCH, 8), pairs), :].astype(jnp.bfloat16)
                for k in range(2)
            ]
            out = jnp.dot(
                matrix[...], jnp.concatenate(pair, 1), preferred_element_type=jnp.float32
            )
            for k in range(2):
                for v in range(width):
                    rows[pl.ds(v * outs * capacity + a + k, outs, stride=capacity), :] = out[
                        v * outs : (v + 1) * outs, k * 128 : (k + 1) * 128
                    ]
        return 0

    lax.fori_loop(0, capacity // UNROLL, apply, 0)

    def finish(t, _):
        pieces = [
            rows[pl.ds(pl.multiple_of((v * outs + t) * capacity, 8), capacity), :][:, :capacity]
            for v in range(width)
        ]
        joined = jnp.concatenate(pieces, 1)
        theta[t] = jnp.where(live[t] > 0.5, joined, 0.0).astype(theta.dtype)
        return 0

    lax.fori_loop(0, theta.shape[0], finish, 0)


PITCH = 200
UNROLL = 8


def make_theta(carry, matrix, live, sites):
    width, capacity = carry.shape[0], carry.shape[1]
    phys = live.shape[0]
    vmem = pl.BlockSpec(memory_space=pltpu.VMEM)
    return pl.pallas_call(
        theta_kernel,
        out_shape=jax.ShapeDtypeStruct((phys, capacity, width * capacity), jnp.bfloat16),
        in_specs=[vmem] * (3 + len(sites)),
        out_specs=vmem,
        scratch_shapes=[
            pltpu.VMEM((PITCH * capacity, 128), jnp.float32),
            pltpu.VMEM((matrix.shape[0] * capacity, 128), jnp.float32),
        ],
        compiler_params=pltpu.CompilerParams(vmem_limit_bytes=48 * 1024 * 1024),
        name="theta",
    )(carry, matrix, live, *sites)


def body(carry, site, mpo, omega, sector_sizes):
    count = lax.axis_size("sec")
    sector = lax.axis_index("sec")
    capacity = carry.shape[1]
    bond_width = mpo.shape[0]
    phys_width = mpo.shape[1]
    raw = site[0]
    phys_up, phys_down, bond_up, bond_down = charge_tables()
    rows = jnp.arange(capacity, dtype=jnp.int32)
    paired = count == 2 * GRID_DN
    operator = jnp.where(jnp.asarray(conserving()), mpo, jnp.zeros_like(mpo))

    def theta_at(base, carry_block, sites, first, taken, padded):
        def sizes_at(up, down):
            at = jnp.clip(base + jnp.asarray(up * GRID_DN + down), 0, count - 1)
            hit = at[..., None] == jnp.arange(count, dtype=jnp.int32)
            found = jnp.sum(jnp.where(hit, sector_sizes, 0), -1)
            return jnp.where(inside(base, up, down, count), found, 0)

        own_size = sizes_at(np.zeros((1,), np.int32), np.zeros((1,), np.int32))
        source_sizes = sizes_at(-bond_up, -bond_down)
        carry_live = (rows[None, :, None] < own_size) & (
            rows[None, None, :] < source_sizes[:, None, None]
        )
        carry_three = carry_block.reshape(capacity, bond_width, capacity).transpose(1, 0, 2)
        carry_three = jnp.where(carry_live, carry_three, jnp.zeros_like(carry_three))
        column_sizes = sizes_at(
            phys_up[:, None] - bond_up[None, :], phys_down[:, None] - bond_down[None, :]
        )
        target_ok = inside(base, phys_up, phys_down, count)
        live = (rows[None, None, :] < column_sizes[:, :, None]) & target_ok[:, None, None]
        live = live.astype(jnp.float32).reshape(phys_width, 1, bond_width * capacity)
        live = lax.dynamic_slice_in_dim(live, first, taken, 0)
        used = lax.dynamic_slice_in_dim(operator, first, taken, 1)
        used = jnp.pad(used, ((0, 0), (0, padded - taken), (0, 0), (0, 0)))
        matrix = used.transpose(3, 1, 0, 2).reshape(
            padded * bond_width, phys_width * bond_width
        )
        return make_theta(carry_three, matrix, live, sites)

    if paired:
        swap = [(i, (i + GRID_DN) % count) for i in range(count)]
        other = lax.rem(sector + GRID_DN, count)
        site_other = lax.ppermute(raw, "sec", swap)
        carry_other = lax.ppermute(carry[0], "sec", swap)

        def along(value, step):
            moves = [
                (i, i + step) for i in range(count) if 0 <= i % GRID_DN + step < GRID_DN
            ]
            return lax.ppermute(value, "sec", moves)

        sites = [raw, site_other, site_other, along(raw, 1), along(raw, -1)]
        others = [site_other, raw, raw, along(site_other, 1), along(site_other, -1)]
        side = phys_width // 4
        entry = (sector // GRID_DN) * (phys_width - side)
        thetas = [
            theta_at(sector, carry[0], sites, side, phys_width - 2 * side, phys_width - 2 * side),
            theta_at(other, carry_other, others, entry, side, 2 * side),
        ]
    else:
        sites = [raw] + [
            shifted(raw, "sec", up * GRID_DN + down) for _, _, up, down in GROUPS[1:]
        ]
        thetas = [theta_at(sector, carry[0], sites, 0, phys_width, phys_width)]
    left, next_carry = solve(thetas, omega, count, phys_width)
    return (left.reshape(1, phys_width, capacity, omega.shape[1]), next_carry[None])


def solution(mesh):
    return jax.shard_map(
        body,
        mesh=mesh,
        in_specs=(
            P(("parts", "sec"), None, None),
            P(("parts", "sec"), None, None),
            P("parts", None, None, None),
            P(),
            P("parts"),
        ),
        out_specs=(P(("parts", "sec"), None, None, None), P(("parts", "sec"), None, None)),
        check_vma=False,
    )
```
